64 devices in a mesh: dp: 4 (over x, y), ep: 16 (over z, core).
Axes of the slice: x: 2, y: 2, z: 8, core: 2. Of those that a mesh axis runs over, the one named last changes fastest.
The devices are a block of a 4x4x8 slice.
Arguments:
- hidden: bfloat16 [16384, 2048], P(('dp', 'ep')), parts along dimension 0
- router_w: float32 [2048, 16], replicated
- expert_ids: int32 [16384, 2], P(('dp', 'ep')), parts along dimension 0
- w_gate: bfloat16 [16, 2048, 3200], P('ep')
- w_up: bfloat16 [16, 2048, 3200], P('ep')
- w_down: bfloat16 [16, 3200, 2048], P('ep')
- post_scale: float32 [2], replicated
Outputs:
- output: bfloat16 [16384, 2048], P(('dp', 'ep')), parts along dimension 0
There are 4 independent parts. The reference program is written for one: setup_inputs(seed, part) draws one part's arguments, and reference() takes and returns one part's arrays. A program takes and returns all parts, laid end to end along the dimension named above; an argument that names none is the same for every part.
All inputs are finite; a program needn't handle non-finite values.
Results may differ from the reference program's by a relative error of at most 0.001.
Values are sent between devices in bfloat16 or wider.
A program may use at most 768 MiB of HBM per device.

```python
import jax
import jax.numpy as jnp
from jax import lax

GROUP_SIZE = 16
TOKENS_DEV = 256
EXPERTS = 16
HIDDEN = 2048
FFN_DIM = 3200
TOP_K = 2
BATCH_ROWS = GROUP_SIZE * TOKENS_DEV
HOT_COUNT = max(1, EXPERTS // 8)
CAPACITY = TOKENS_DEV // HOT_COUNT
MAX_ROWS = GROUP_SIZE * CAPACITY


def draw_routing(ids_key, part):
    order_key, shard_key = jax.random.split(ids_key)
    expert_order = jax.random.permutation(order_key, EXPERTS)
    hot_ids = expert_order[:HOT_COUNT]
    cold_ids = expert_order[HOT_COUNT:]
    shard_keys = jax.random.split(jax.random.fold_in(shard_key, part), GROUP_SIZE)

    def one_shard(one_key):
        tok_key, cold_key, swap_key = jax.random.split(one_key, 3)
        tok_rank = jax.random.permutation(tok_key, TOKENS_DEV)
        cold_mix = jax.random.permutation(cold_key, cold_ids)
        first_pick = hot_ids[tok_rank % HOT_COUNT]
        second_pick = cold_mix[tok_rank % (EXPERTS - HOT_COUNT)]
        swapped = jax.random.randint(swap_key, (TOKENS_DEV,), 0, 2) == 1
        return jnp.stack([jnp.where(swapped, second_pick, first_pick), jnp.where(swapped, first_pick, second_pick)], axis=1)

    return jax.vmap(one_shard)(shard_keys).reshape(BATCH_ROWS, TOP_K).astype(jnp.int32)


def draw_experts(weight_key, row_count, col_count):
    expert_keys = jax.random.split(weight_key, EXPERTS)
    return lax.map(lambda one_key: (jax.random.normal(one_key, (row_count, col_count), jnp.float32) * row_count ** -0.5).astype(jnp.bfloat16), expert_keys)


def setup_inputs(seed: int = 0, part: int = 0) -> dict:
    base_key = jax.random.key(seed)
    hid_key, route_key, gate_key, up_key, down_key, post_key, ids_key = jax.random.split(base_key, 7)
    hidden = jax.random.normal(jax.random.fold_in(hid_key, part), (BATCH_ROWS, HIDDEN), jnp.float32).astype(jnp.bfloat16)
    router_w = jax.random.normal(route_key, (HIDDEN, EXPERTS), jnp.float32) * (0.4 * HIDDEN ** -0.5)
    w_gate = draw_experts(gate_key, HIDDEN, FFN_DIM)
    w_up = draw_experts(up_key, HIDDEN, FFN_DIM)
    w_down = draw_experts(down_key, FFN_DIM, HIDDEN)
    post_scale = jax.random.uniform(post_key, (2,), jnp.float32, jnp.array([0.5, 1.0], jnp.float32), jnp.array([1.0, 2.0], jnp.float32))
    expert_ids = draw_routing(ids_key, part)
    return {'hidden': hidden, 'router_w': router_w, 'expert_ids': expert_ids, 'w_gate': w_gate, 'w_up': w_up, 'w_down': w_down, 'post_scale': post_scale}


def reference(hidden, router_w, expert_ids, w_gate, w_up, w_down, post_scale):
    hid_wide = hidden.astype(jnp.float32)
    logits = jnp.dot(hid_wide, router_w, preferred_element_type=jnp.float32)
    router_prob = jax.nn.softmax(logits, axis=-1)
    picked = jnp.take_along_axis(router_prob, expert_ids, axis=1)
    gates = picked / jnp.sum(picked, axis=1, keepdims=True)

    def add_expert(running_sum, expert):
        hit_mask = expert_ids == expert
        tok_gate = jnp.sum(jnp.where(hit_mask, gates, 0.0), axis=1)
        chosen = jnp.any(hit_mask, axis=1)
        row_index = jnp.nonzero(chosen, size=MAX_ROWS, fill_value=0)[0]
        in_range = jnp.arange(MAX_ROWS) < jnp.sum(chosen)
        tok_rows = hidden[row_index]
        gate_in = jnp.dot(tok_rows, w_gate[expert], preferred_element_type=jnp.float32)
        up_in = jnp.dot(tok_rows, w_up[expert], preferred_element_type=jnp.float32)
        middle = (jax.nn.silu(gate_in) * up_in).astype(jnp.bfloat16)
        expert_out = jnp.dot(middle, w_down[expert], preferred_element_type=jnp.float32).astype(jnp.bfloat16)
        row_weight = jnp.where(in_range, tok_gate[row_index], 0.0)
        running_sum = running_sum.at[row_index].add(row_weight[:, None] * expert_out.astype(jnp.float32))
        return running_sum, None

    mixed, _ = lax.scan(add_expert, jnp.zeros((BATCH_ROWS, HIDDEN), jnp.float32), jnp.arange(EXPERTS))
    return (post_scale[0] * hid_wide + post_scale[1] * mixed).astype(jnp.bfloat16)
```

```python
import functools

import jax
import jax.numpy as jnp
from jax import lax
from jax.experimental import pallas as pl
from jax.experimental.pallas import tpu as pltpu
from jax.sharding import PartitionSpec as P

MESH = pl.DeviceIdType.MESH
SUBS = 4
DIRECT = 24
PITCH = 32
F32, BF16 = jnp.float32, jnp.bfloat16


def tiles(width, size):
    return [(off, min(size, width - off)) for off in range(0, width, size)]


def moe_kernel(ep, cap, hid, rwt, idt, w1, w3, w2, ps, out, flag, agr, ags,
               w1v, w3v, w2v, xr, xs, xsel, mid, ycat, ysib, rs, sec, tmat, cr, cs, gat,
               w1s, w3s, w2s, ldr, lds, agsend, agrecv, sibsend, sibrecv,
               cse, crv, sse, srv, yss, ysr, s1s, s2s, secr, rss, rsr, outs):
    tokens, width = hid.shape
    ffn = w1.shape[2]
    chips = ep // 2
    sub = tokens // SUBS
    me = lax.axis_index('ep')
    chip, core = me // 2, lax.rem(me, 2)
    way = 1 - 2 * core
    sib = me + way
    d_tiles, f_tiles = tiles(width, 512), tiles(ffn, 512)

    def on_chip(steps):
        return lax.rem(chip + steps * way + chips, chips)

    nxt = on_chip(1) * 2 + core

    def rows(q):
        return pl.ds(q * sub, sub)

    def dev(i):
        return dict(device_id={'ep': i}, device_id_type=MESH)

    def ring_sub(k, q, first=False):
        src = hid.at[rows(q)] if first else agr.at[k, rows(q)]
        return pltpu.make_async_remote_copy(src, agr.at[k + 1, rows(q)], agsend.at[k, q], agrecv.at[k + 1, q], **dev(nxt))

    def sib_sub(k, q, first=False):
        src = hid.at[rows(q)] if first else agr.at[k, rows(q)]
        return pltpu.make_async_remote_copy(src, ags.at[k, rows(q)], sibsend.at[k, q], sibrecv.at[k, q], **dev(sib))

    def code_ring(k):
        return pltpu.make_async_remote_copy(cr.at[k], cr.at[k + 1], cse.at[k], crv.at[k + 1], **dev(nxt))

    def code_sib(k):
        return pltpu.make_async_remote_copy(cr.at[k], cs.at[k], sse.at[k], srv.at[k], **dev(sib))

    def load_r(k, q, first=False):
        src = hid.at[rows(q)] if first else agr.at[k, rows(q)]
        return pltpu.make_async_copy(src, xr.at[rows(q)], ldr.at[q])

    def load_s(k, q):
        return pltpu.make_async_copy(ags.at[k, rows(q)], xs.at[rows(q)], lds.at[q])

    def y_copy(k):
        return pltpu.make_async_remote_copy(ysib.at[lax.rem(k, 2)], ycat.at[k, pl.ds(cap, cap)], yss.at[k], ysr.at[k], **dev(sib))

    def slot(e):
        return sec.at[pl.ds(pl.multiple_of(e * PITCH, PITCH), DIRECT)]

    def direct_r(k):
        return pltpu.make_async_remote_copy(ycat.at[k, pl.ds(0, DIRECT)], slot(me), s1s.at[k], secr.at[me], **dev(on_chip(-k) * 2 + core))

    def direct_s(k):
        return pltpu.make_async_remote_copy(ysib.at[lax.rem(k, 2), pl.ds(0, DIRECT)], slot(me), s2s.at[k], secr.at[me], **dev(on_chip(k) * 2 + 1 - core))

    def rs_copy(k, q, first=False):
        src = xsel.at[rows(q)] if first else rs.at[k - 2, rows(q)]
        return pltpu.make_async_remote_copy(src, rs.at[k - 1, rows(q)], rss.at[k, q], rsr.at[k + 1, q], **dev(nxt))

    def rs_arrival(k, q):
        return pltpu.make_async_remote_copy(xsel.at[rows(q)], rs.at[k - 2, rows(q)], rss.at[k - 1, q], rsr.at[k, q], **dev(nxt))

    def load_up(i):
        off, size = f_tiles[i]
        cols = pl.ds(off, size)
        return (pltpu.make_async_copy(w1.at[0, :, cols], w1v.at[:, cols], w1s.at[i]),
                pltpu.make_async_copy(w3.at[0, :, cols], w3v.at[:, cols], w3s.at[i]))

    def load_down(i):
        off, size = d_tiles[i]
        cols = pl.ds(off, size)
        return pltpu.make_async_copy(w2.at[0, :, cols], w2v.at[:, cols], w2s.at[i])

    for q in range(SUBS):
        load_r(0, q, True).start()
    for i in range(len(f_tiles)):
        for copy in load_up(i):
            copy.start()
    for i in range(len(d_tiles)):
        load_down(i).start()
    sec[...] = jnp.zeros_like(sec)

    barrier = pltpu.get_barrier_semaphore()
    for d in range(1, ep):
        pl.semaphore_signal(barrier, inc=1, **dev(lax.rem(me + d, ep)))
    pl.semaphore_wait(barrier, ep - 1)

    for q in range(SUBS):
        ring_sub(0, q, True).start()
    for q in range(SUBS):
        sib_sub(0, q, True).start()

    row0, row1 = idt[0:1, :], idt[1:2, :]
    eio = lax.broadcasted_iota(jnp.int32, (ep, tokens), 0)
    m0 = jnp.where(eio == row0, 1.0, 0.0)
    m1 = jnp.where(eio == row1, 1.0, 0.0)
    cnt = jnp.sum(m0 + m1, axis=1, keepdims=True)
    lead = jnp.broadcast_to(jnp.sum((m0 - m1) * cnt, axis=0, keepdims=True), (ep, tokens))
    mp = jnp.where(lead >= 0, m0, m1)
    ms = m0 + m1 - mp
    earlier = jnp.where(lax.broadcasted_iota(jnp.int32, (tokens, tokens), 0) < lax.broadcasted_iota(jnp.int32, (tokens, tokens), 1), 1.0, 0.0).astype(BF16)
    rank_p = jnp.dot(mp.astype(BF16), earlier, preferred_element_type=F32)
    rank_s = jnp.dot(ms.astype(BF16), earlier, preferred_element_type=F32)
    n_s = jnp.sum(ms, axis=1, keepdims=True)
    ef = eio.astype(F32)
    code_p = jnp.sum(mp * (ef * cap + n_s + rank_p), axis=0, keepdims=True)
    code_s = jnp.sum(ms * (ef * cap + rank_s), axis=0, keepdims=True)
    place_s = jnp.sum(ms * (ef * PITCH + rank_s), axis=0, keepdims=True)
    r8 = lax.broadcasted_iota(jnp.int32, (8, tokens), 0)
    cr[0] = jnp.where(r8 == 0, code_p, jnp.where(r8 == 1, code_s, 0.0))

    for q in range(SUBS):
        load_r(0, q, True).wait()
    code_ring(0).start()
    code_sib(0).start()
    logits = jnp.zeros((ep, tokens), F32)
    for off, size in d_tiles:
        logits += lax.dot_general(rwt[:, off:off + size], xr[:, off:off + size].astype(F32), (((1,), (1,)), ((), ())),
                                  precision=lax.Precision.HIGHEST, preferred_element_type=F32)
    grown = jnp.exp(logits - jnp.max(logits, axis=0, keepdims=True))
    prob = grown / jnp.sum(grown, axis=0, keepdims=True)
    prob_p = jnp.sum(mp * prob, axis=0, keepdims=True)
    prob_s = jnp.sum(ms * prob, axis=0, keepdims=True)
    total = prob_p + prob_s
    r128 = lax.broadcasted_iota(jnp.int32, (128, tokens), 0)
    gat[...] = jnp.where(r128 == 0, prob_p / total, jnp.where(r128 == 1, prob_s / total, jnp.where(r128 == 2, place_s, 0.0))).T

    for q in range(SUBS):
        sib_sub(0, q, True).wait_recv()
        load_s(0, q).start()
    for q in range(SUBS):
        load_s(0, q).wait()
    code_sib(0).wait_recv()

    mine = (me * cap).astype(F32) + lax.broadcasted_iota(jnp.int32, (cap, tokens), 0).astype(F32)

    def pick(codes, block, base):
        hot = jnp.where((codes[0:1, :] == mine) | (codes[1:2, :] == mine), 1.0, 0.0).astype(BF16)
        for off, size in d_tiles:
            xsel[base:base + cap, off:off + size] = jnp.dot(hot, block[:, off:off + size], preferred_element_type=F32).astype(BF16)

    def poll(k, q):
        if q < SUBS:
            ring_sub(k - 1, q).wait_recv()

            @pl.when(k < chips - 1)
            def _():
                ring_sub(k, q).start()
            sib_sub(k, q).start()
            load_r(k, q).start()
        if q == 0:
            code_ring(k - 1).wait_recv()

            @pl.when(k < chips - 1)
            def _():
                code_ring(k).start()
            code_sib(k).start()
        if q > 0:
            sib_sub(k, q - 1).wait_recv()
            load_s(k, q - 1).start()
        if q == SUBS:
            code_sib(k).wait_recv()

    up_count = len(f_tiles)
    pieces = up_count + len(d_tiles)
    poll_at = {}
    for q in range(SUBS + 1):
        poll_at.setdefault(min(pieces - 1, (q + 1) * pieces // (SUBS + 1) - 1), []).append(q)

    def expert_step(k, carry):
        @pl.when(k > 0)
        def _():
            for q in range(SUBS):
                load_r(k, q).wait()
                load_s(k, q).wait()
        pick(cr[k], xr, 0)
        pick(cs[k], xs, cap)

        @pl.when(k >= 2)
        def _():
            y_copy(k - 2).wait_send()
            direct_s(k - 2).wait_send()
        for piece in range(pieces):
            if piece < up_count:
                off, size = f_tiles[piece]

                @pl.when(k == 0)
                def _():
                    for copy in load_up(piece):
                        copy.wait()
                gate = jnp.dot(xsel[...], w1v[:, off:off + size], preferred_element_type=F32)
                up = jnp.dot(xsel[...], w3v[:, off:off + size], preferred_element_type=F32)
                mid[:, off:off + size] = (jax.nn.silu(gate) * up).astype(BF16)
            else:
                off, size = d_tiles[piece - up_count]

                @pl.when(k == 0)
                def _():
                    load_down(piece - up_count).wait()
                y = jnp.dot(mid[...], w2v[:, off:off + size], preferred_element_type=F32).astype(BF16)
                ycat[k, 0:cap, off:off + size] = y[:cap]
                ysib[lax.rem(k, 2), :, off:off + size] = y[cap:]
            for q in poll_at.get(piece, []):
                @pl.when(k < chips - 1)
                def _():
                    poll(k + 1, q)
        y_copy(k).start()
        direct_s(k).start()

        @pl.when(k > 0)
        def _():
            direct_r(k).start()
        return carry

    lax.fori_loop(0, chips, expert_step, 0)

    for q in range(SUBS):
        load_r(0, q, True).start()
    s_io = lax.broadcasted_iota(jnp.int32, (2 * cap, tokens), 0)
    pair = jnp.where(s_io < cap, me * cap + s_io, sib * cap + s_io - cap).astype(F32)

    def place(k):
        tmat[...] = jnp.where(cr[k][0:1, :] == pair, 1.0, 0.0).T.astype(BF16)

    place(1)
    y_copy(1).wait_recv()
    for q in range(SUBS):
        for off, size in d_tiles:
            xsel[q * sub:(q + 1) * sub, off:off + size] = jnp.dot(
                tmat[q * sub:(q + 1) * sub, :], ycat[1, :, off:off + size], preferred_element_type=F32).astype(BF16)
        rs_copy(1, q, True).start()

    def ring_step(k, carry):
        place(k)
        y_copy(k).wait_recv()
        for q in range(SUBS):
            rs_arrival(k, q).wait_recv()
            for off, size in d_tiles:
                part = jnp.dot(tmat[q * sub:(q + 1) * sub, :], ycat[k, :, off:off + size], preferred_element_type=F32)
                old = rs[k - 2, q * sub:(q + 1) * sub, off:off + size]
                rs[k - 2, q * sub:(q + 1) * sub, off:off + size] = (part + old.astype(F32)).astype(BF16)
            rs_copy(k, q).start()
        return carry

    lax.fori_loop(2, chips, ring_step, 0)

    for k in (chips - 2, chips - 1):
        y_copy(k).wait_send()
        direct_s(k).wait_send()
    worst = jnp.zeros((1, tokens), F32)
    for k in range(chips):
        for codes in (cr, cs):
            code = codes[k][1:2, :]
            worst = jnp.maximum(worst, code - jnp.floor(code * (1.0 / cap)) * cap)
    flag[...] = jnp.broadcast_to(jnp.max(worst, axis=1, keepdims=True), flag.shape)

    place(0)
    y_copy(0).wait_recv()
    sec[pl.ds(pl.multiple_of(me * PITCH, PITCH), DIRECT), :] = ycat[0, 0:DIRECT, :]
    for e in range(ep):
        @pl.when(me != e)
        def _():
            pltpu.make_async_remote_copy(ycat.at[0, pl.ds(0, DIRECT)], slot(e), s1s.at[0], secr.at[e], **dev(sib)).wait_recv()
    lanes = lax.broadcasted_iota(jnp.int32, (tokens, ep * PITCH), 1).astype(F32)
    sel = jnp.where(lanes == gat[:, 2:3], 1.0, 0.0).astype(BF16)
    for off, size in d_tiles:
        got = jnp.dot(sel, sec[:, off:off + size], preferred_element_type=F32).astype(BF16)
        for half in range(2):
            ysib[half, :, off:off + size] = got[half * cap:(half + 1) * cap]
    for q in range(SUBS):
        load_r(0, q, True).wait()
    alpha, beta = ps[0], ps[1]
    per_half = cap // sub
    for q in range(SUBS):
        rs_arrival(chips, q).wait_recv()
        at = slice(q * sub, (q + 1) * sub)
        base = (q % per_half) * sub
        for off, size in d_tiles:
            cols = slice(off, off + size)
            main = jnp.dot(tmat[at, :], ycat[0, :, cols], preferred_element_type=F32) + rs[chips - 2, at, cols].astype(F32)
            other = ysib[q // per_half, base:base + sub, cols].astype(F32)
            mixed = gat[at, 0:1] * main + gat[at, 1:2] * other
            xs[at, cols] = (alpha * xr[at, cols].astype(F32) + beta * mixed).astype(BF16)
        pltpu.make_async_copy(xs.at[rows(q)], out.at[rows(q)], outs.at[q]).start()

    def drain(k, carry):
        for q in range(SUBS):
            @pl.when(k < chips - 1)
            def _():
                ring_sub(k, q).wait_send()
            sib_sub(k, q).wait_send()

            @pl.when(k > 0)
            def _():
                rs_arrival(k + 1, q).wait_send()

        @pl.when(k < chips - 1)
        def _():
            code_ring(k).wait_send()
        code_sib(k).wait_send()

        @pl.when(k > 0)
        def _():
            direct_r(k).wait_send()
        return carry

    lax.fori_loop(0, chips, drain, 0)
    for q in range(SUBS):
        pltpu.make_async_copy(xs.at[rows(q)], out.at[rows(q)], outs.at[q]).wait()


def route_tables(hidden, router_w, expert_ids, experts, capacity):
    tokens, choice_count = expert_ids.shape
    logits = jnp.dot(hidden.astype(F32), router_w, precision=lax.Precision.HIGHEST, preferred_element_type=F32)
    router_prob = jax.nn.softmax(logits, axis=-1)
    pick_mask = expert_ids[:, :, None] == jnp.arange(experts, dtype=jnp.int32)[None, None, :]
    picked = jnp.sum(jnp.where(pick_mask, router_prob[:, None, :], 0.0), axis=-1)
    gates = picked / jnp.sum(picked, axis=1, keepdims=True)
    pair_hot = pick_mask.reshape(tokens * choice_count, experts).astype(jnp.int32)
    earlier = jnp.cumsum(pair_hot, axis=0) - pair_hot
    slot_of = jnp.sum(earlier * pair_hot, axis=1).reshape(tokens, choice_count)
    slot_mask = slot_of[:, :, None] == jnp.arange(capacity, dtype=jnp.int32)[None, None, :]
    place = pick_mask[:, :, :, None] & slot_mask[:, :, None, :]
    return gates, place


def padded_step(ep, hidden, router_w, expert_ids, w_gate, w_up, w_down, post_scale):
    tokens, width = hidden.shape
    capacity = tokens // max(1, ep // 8)
    gates, place = route_tables(hidden, router_w, expert_ids, ep, capacity)
    token_table = jnp.any(place, axis=1).astype(BF16)
    outgoing = jnp.einsum('tec,td->ecd', token_table, hidden, preferred_element_type=F32).astype(BF16)
    incoming = lax.all_to_all(outgoing, 'ep', 0, 0, tiled=True).reshape(ep * capacity, width)
    gate_in = jnp.dot(incoming, w_gate[0], preferred_element_type=F32)
    up_in = jnp.dot(incoming, w_up[0], preferred_element_type=F32)
    middle = (jax.nn.silu(gate_in) * up_in).astype(BF16)
    expert_out = jnp.dot(middle, w_down[0], preferred_element_type=F32).astype(BF16)
    returned = lax.all_to_all(expert_out.reshape(ep, capacity, width), 'ep', 0, 0, tiled=True)
    pair_out = jnp.einsum('tkec,ecd->tkd', place.astype(BF16), returned, preferred_element_type=F32)
    mixed = jnp.sum(gates[:, :, None] * pair_out, axis=1)
    result = post_scale[0] * hidden.astype(F32) + post_scale[1] * mixed
    return result.astype(BF16)


def solution(mesh):
    ep = mesh.shape['ep']

    def local_step(hidden, router_w, expert_ids, w_gate, w_up, w_down, post_scale):
        tokens, width = hidden.shape
        ffn = w_gate.shape[2]
        chips = ep // 2
        cap = tokens // max(1, ep // 8)
        anyspace = pl.BlockSpec(memory_space=pl.ANY)
        vmem = pl.BlockSpec(memory_space=pltpu.VMEM)
        dma = pltpu.SemaphoreType.DMA
        n_f, n_d = len(tiles(ffn, 512)), len(tiles(width, 512))
        block = jax.ShapeDtypeStruct((chips, tokens, width), BF16)
        result, flag, _, _ = pl.pallas_call(
            functools.partial(moe_kernel, ep, cap),
            out_shape=(jax.ShapeDtypeStruct((tokens, width), BF16), jax.ShapeDtypeStruct((8, 128), F32), block, block),
            in_specs=[anyspace, vmem, vmem, anyspace, anyspace, anyspace, pl.BlockSpec(memory_space=pltpu.SMEM)],
            out_specs=(anyspace, vmem, anyspace, anyspace),
            scratch_shapes=[
                pltpu.VMEM((width, ffn), BF16), pltpu.VMEM((width, ffn), BF16), pltpu.VMEM((ffn, width), BF16),
                pltpu.VMEM((tokens, width), BF16), pltpu.VMEM((tokens, width), BF16), pltpu.VMEM((2 * cap, width), BF16),
                pltpu.VMEM((2 * cap, ffn), BF16),
                pltpu.VMEM((chips, 2 * cap, width), BF16), pltpu.VMEM((2, cap, width), BF16),
                pltpu.VMEM((chips - 1, tokens, width), BF16), pltpu.VMEM((ep * PITCH, width), BF16),
                pltpu.VMEM((tokens, 2 * cap), BF16),
                pltpu.VMEM((chips, 8, tokens), F32), pltpu.VMEM((chips, 8, tokens), F32), pltpu.VMEM((tokens, 128), F32),
                dma((n_f,)), dma((n_f,)), dma((n_d,)), dma((SUBS,)), dma((SUBS,)),
                dma((chips, SUBS)), dma((chips, SUBS)), dma((chips, SUBS)), dma((chips, SUBS)),
                dma((chips,)), dma((chips,)), dma((chips,)), dma((chips,)),
                dma((chips,)), dma((chips,)), dma((chips,)), dma((chips,)), dma((ep,)),
                dma((chips, SUBS)), dma((chips + 1, SUBS)), dma((SUBS,)),
            ],
            compiler_params=pltpu.CompilerParams(collective_id=0, has_side_effects=True, vmem_limit_bytes=67043328),
            name='moe_ring',
        )(hidden, router_w.T, expert_ids.T, w_gate, w_up, w_down, post_scale)
        return lax.cond(
            flag[0, 0] >= DIRECT,
            lambda: padded_step(ep, hidden, router_w, expert_ids, w_gate, w_up, w_down, post_scale),
            lambda: result)

    tok_spec = P(('dp', 'ep'))
    return jax.shard_map(local_step, mesh=mesh, in_specs=(tok_spec, P(), tok_spec, P('ep'), P('ep'), P('ep'), P()), out_specs=tok_spec, check_vma=False)
```
